32 devices in a mesh: row: 16 (over z, x, core), col: 2 (over y).
Axes of the slice: x: 2, y: 2, z: 4, core: 2. Of those that a mesh axis runs over, the one named last changes fastest.
Arguments:
- occupied_waves: bfloat16 [1024, 32768], P('row', 'col'), may hold values from -6 to 6
- virtual_waves: bfloat16 [512, 32768], P('row', 'col'), may hold values from -6 to 6
- occupied_decay: float32 [1024], replicated, may hold values from 0.02 to 1
- virtual_decay: float32 [512], replicated, may hold values from 0.02 to 1
Outputs:
- spectrum_real: float32 [512, 32, 1024], P('row', 'col')
- spectrum_imaginary: float32 [512, 32, 1024], P('row', 'col')
The draws below stay inside these ranges and needn't reach their ends.
All inputs are finite; a program needn't handle non-finite values.
Results may differ from the reference program's by a relative error of at most 0.0041.
Values may be sent and summed in bfloat16 or wider, within the bound.
A program may use at most 128 MiB of HBM per device.

```python
import math
import jax
import jax.numpy as jnp
from jax import lax

NOCC = 1024
NVIR = 512
NA = 32
NB = 32
NC = 32
ROWS_DEV = 32
NGRID = 32768
N_ROW = 16


def steps_of(key, dims, pieces, smallest, high):
    loudness, own = 1.0, jax.random.fold_in(key, 6)
    for position, parts in pieces:
        heights = jnp.exp(jax.random.uniform(jax.random.fold_in(own, position), (parts,), jnp.float32, smallest / len(pieces), high / len(pieces)))
        loudness = loudness * jnp.repeat(heights, dims[position] // parts).reshape([-1 if axis == position else 1 for axis in range(len(dims))])
    return loudness


def noise(rng, extent, scale, limit, split=(), kind=jnp.bfloat16):
    drawn = scale * jax.random.normal(rng, extent, jnp.float32)
    if split:
        drawn = drawn * steps_of(rng, extent, split, -0.22, 0.18)
    return jnp.clip(drawn, -limit, limit).astype(kind)


def setup_inputs(seed: int = 0) -> dict:
    keys = jax.random.split(jax.random.key(seed), 5)
    return {
        "occupied_waves": noise(keys[0], (NOCC, NGRID), 1.0, 6.0, ((0, 16), (1, 2))),
        "virtual_waves": noise(keys[1], (NVIR, NGRID), 1.0, 6.0, ((0, 16), (1, 2))),
        "occupied_decay": jnp.clip(jnp.exp(jax.random.uniform(keys[2], (NOCC,), jnp.float32, math.log(0.02), math.log(1.0))), 0.02, 1.0),
        "virtual_decay": jnp.clip(jnp.exp(jax.random.uniform(keys[3], (NVIR,), jnp.float32, math.log(0.02), math.log(1.0))), 0.02, 1.0),
    }


def reference(occupied_waves, virtual_waves, occupied_decay, virtual_decay):
    rows_all = ROWS_DEV * N_ROW
    width = math.gcd(rows_all, 512)
    factor = -1.0 / math.sqrt(NOCC * NVIR)
    contract = (((0,), (0,)), ((), ()))

    def block(index):
        first = (index * width).astype(jnp.int32)
        occ_rows = lax.dynamic_slice_in_dim(occupied_waves, first, width, 1)
        occ_rows = (occ_rows.astype(jnp.float32) * occupied_decay[:, None]).astype(jnp.bfloat16)
        vir_rows = lax.dynamic_slice_in_dim(virtual_waves, first, width, 1)
        vir_rows = (vir_rows.astype(jnp.float32) * virtual_decay[:, None]).astype(jnp.bfloat16)
        green_occ = lax.dot_general(occupied_waves, occ_rows, contract, preferred_element_type=jnp.float32)
        green_vir = lax.dot_general(virtual_waves, vir_rows, contract, preferred_element_type=jnp.float32)
        polar = green_occ * green_vir * factor
        cube = polar.reshape(NA, NB, NC, width)
        spectrum = jnp.fft.fftn(cube, axes=(0, 1, 2)) / math.sqrt(NGRID)
        spectrum = jnp.transpose(spectrum, (3, 2, 0, 1)).reshape(width, NC, NA * NB)
        return (jnp.real(spectrum).astype(jnp.float32), jnp.imag(spectrum).astype(jnp.float32))
    real_part, imag_part = lax.map(block, jnp.arange(rows_all // width, dtype=jnp.int32))
    real_part = real_part.reshape(rows_all, NC, NA * NB)
    imag_part = imag_part.reshape(rows_all, NC, NA * NB)
    return (real_part, imag_part)
```

```python
import functools
import math

import jax
import jax.numpy as jnp
import numpy as np
from jax import lax
from jax.experimental import pallas as pl
from jax.experimental.pallas import tpu as pltpu
from jax.sharding import PartitionSpec as P

NA = 32
NB = 32
NC = 32
NAB = NA * NB
NGRID = NA * NB * NC
LANES = 128
R_BLOCK = 16


def trig(phase, length):
    angle = (phase % length) * (2.0 * math.pi / length)
    return np.cos(angle), np.sin(angle)


def bf16_table(table):
    return jnp.asarray(table.astype(np.float32)).astype(jnp.bfloat16)


def plane_tables():
    index = np.arange(NAB)
    a, b = index // NB, index % NB
    phase = a[:, None] * a[None, :] * NB + b[:, None] * b[None, :] * NA
    cosine, sine = trig(phase, NA * NB)
    return bf16_table(cosine), bf16_table(sine)


def line_tables(col_count):
    share = NC // col_count
    full = np.zeros((col_count, 2, R_BLOCK, share, NC, R_BLOCK))
    for y in range(col_count):
        kc = y * share + np.arange(share)
        cosine, sine = trig(kc[:, None] * np.arange(NC)[None, :], NC)
        for r in range(R_BLOCK):
            full[y, 0, r, :, :, r] = cosine
            full[y, 1, r, :, :, r] = -sine
    return bf16_table(full.reshape(col_count, 2 * R_BLOCK * share, NC * R_BLOCK))


def swap_table(outer, inner, width):
    index = np.arange(outer * inner * width).reshape(outer, inner, width)
    source = np.transpose(index, (1, 0, 2)).reshape(-1)
    table = np.zeros((source.size, source.size))
    table[source, np.arange(source.size)] = 1.0
    return bf16_table(table)


def dot(a, b):
    return jnp.dot(a, b, preferred_element_type=jnp.float32)


def spectrum_kernel(pieces, x_ref, swap_ref, line_ref, cos_ref, sin_ref, re_ref, im_ref, rows):
    if pieces:
        per = LANES // NB
        for g in range(NA // per):
            parts = []
            for t in range(NC // per):
                lanes = pl.ds(t * LANES, LANES)
                parts.append(
                    jnp.concatenate([x_ref[g * per + k, :, lanes] for k in range(per)], axis=1)
                )
            moved = dot(jnp.concatenate(parts, axis=0), swap_ref[...]).astype(jnp.bfloat16)
            for t in range(NC // per):
                for j in range(per):
                    rows[pl.ds((t * per + j) * R_BLOCK, R_BLOCK), pl.ds(g * LANES, LANES)] = moved[
                        t * R_BLOCK : (t + 1) * R_BLOCK, j * LANES : (j + 1) * LANES
                    ]
    else:
        rows[...] = x_ref[...].reshape(NC * R_BLOCK, NAB)
    line = dot(line_ref[...], rows[...]).astype(jnp.bfloat16)
    half = line.shape[0] // 2
    re, im = line[:half], line[half:]
    re_ref[...] = dot(re, cos_ref[...]) + dot(im, sin_ref[...])
    im_ref[...] = dot(im, cos_ref[...]) - dot(re, sin_ref[...])


def spectrum(pieces, x, line_table):
    r_count = x.shape[1]
    cosine, sine = plane_tables()
    per = LANES // NB
    swap = swap_table(per, per, NB)
    out_rows = line_table.shape[0] // 2
    steps = r_count // R_BLOCK
    whole = lambda table: pl.BlockSpec(table.shape, lambda i: (0, 0))
    out = jax.ShapeDtypeStruct((out_rows * steps, NAB), jnp.float32)
    out_spec = pl.BlockSpec((out_rows, NAB), lambda i: (i, 0))
    return pl.pallas_call(
        functools.partial(spectrum_kernel, pieces),
        grid=(steps,),
        in_specs=[
            pl.BlockSpec((x.shape[0], R_BLOCK, x.shape[2]), lambda i: (0, i, 0)),
            whole(swap),
            whole(line_table),
            whole(cosine),
            whole(sine),
        ],
        out_specs=[out_spec, out_spec],
        out_shape=[out, out],
        scratch_shapes=[pltpu.VMEM((NC * R_BLOCK, NAB), jnp.bfloat16)],
        compiler_params=pltpu.CompilerParams(vmem_limit_bytes=48 * 1024 * 1024),
    )(x, swap, line_table, cosine, sine)


def on_device(rows_dev, occupied_waves, virtual_waves, occupied_decay, virtual_decay):
    row_count = lax.axis_size("row")
    col_count = lax.axis_size("col")
    occ_share = occupied_waves.shape[0]
    share = occ_share + virtual_waves.shape[0]
    nocc, nvir = occupied_decay.shape[0], virtual_decay.shape[0]
    window = rows_dev * row_count
    points = occupied_waves.shape[1] // row_count
    contract = (((0,), (0,)), ((), ()))
    factor = -1.0 / math.sqrt(nocc * nvir) / math.sqrt(NGRID)

    first = jnp.concatenate([occupied_waves[:, :window], virtual_waves[:, :window]], axis=0)
    first = lax.all_gather(first, "col")[0]
    first = lax.all_gather(first, "row")

    def exchange(waves):
        shaped = waves.reshape(waves.shape[0], row_count, points)
        shaped = lax.all_to_all(shaped, "row", split_axis=1, concat_axis=0, tiled=True)
        return shaped.reshape(waves.shape[0] * row_count, points)

    plane_occ = exchange(occupied_waves)
    plane_vir = exchange(virtual_waves)

    def scaled(rows, decay):
        rows = rows.reshape(decay.shape[0], window).astype(jnp.float32)
        return (rows * decay[:, None]).astype(jnp.bfloat16)

    occ_rows = scaled(first[:, :occ_share], occupied_decay)
    vir_rows = scaled(first[:, occ_share:], virtual_decay)
    green_occ = lax.dot_general(occ_rows, plane_occ, contract, preferred_element_type=jnp.float32)
    green_vir = lax.dot_general(vir_rows, plane_vir, contract, preferred_element_type=jnp.float32)
    polar = (green_occ * green_vir * factor).astype(jnp.bfloat16)
    polar = dot(polar, swap_table(points // NC, NC, 1)).astype(jnp.bfloat16)
    polar = polar.reshape(row_count, rows_dev, points)
    polar = lax.all_to_all(polar, "row", split_axis=0, concat_axis=0, tiled=True)
    polar = lax.all_gather(polar, "col")
    pieces = points == NB * NC
    if pieces:
        x = polar.reshape(col_count * row_count, rows_dev, points)
    else:
        x = polar.reshape(col_count * row_count, rows_dev, NC, points // NC)
        x = jnp.transpose(x, (2, 1, 0, 3)).reshape(NC, rows_dev, NAB)
    table = lax.dynamic_index_in_dim(line_tables(col_count), lax.axis_index("col"), 0, False)
    real_part, imag_part = spectrum(pieces, x, table)
    shape = (rows_dev, NC // col_count, NAB)
    return real_part.reshape(shape), imag_part.reshape(shape)


ROWS_DEV = 32


def solution(mesh):
    in_specs = (P("row", "col"), P("row", "col"), P(), P())
    out_specs = (P("row", "col", None), P("row", "col", None))
    return jax.shard_map(
        functools.partial(on_device, ROWS_DEV),
        mesh=mesh,
        in_specs=in_specs,
        out_specs=out_specs,
        check_vma=False,
    )
```

```python
import functools
import math

import jax
import jax.numpy as jnp
import numpy as np
from jax import lax
from jax.experimental import pallas as pl
from jax.experimental.pallas import tpu as pltpu
from jax.sharding import PartitionSpec as P

NA = 32
NB = 32
NC = 32
NAB = NA * NB
NGRID = NA * NB * NC
LANES = 128
R_BLOCK = 16


def trig(phase, length):
    angle = (phase % length) * (2.0 * math.pi / length)
    return np.cos(angle), np.sin(angle)


def bf16_table(table):
    return jnp.asarray(table.astype(np.float32)).astype(jnp.bfloat16)


def plane_tables():
    index = np.arange(NAB)
    a, b = index // NB, index % NB
    phase = a[:, None] * a[None, :] * NB + b[:, None] * b[None, :] * NA
    cosine, sine = trig(phase, NA * NB)
    return bf16_table(cosine), bf16_table(sine)


def line_tables(col_count):
    share = NC // col_count
    full = np.zeros((col_count, 2, R_BLOCK, share, NC, R_BLOCK))
    for y in range(col_count):
        kc = y * share + np.arange(share)
        cosine, sine = trig(kc[:, None] * np.arange(NC)[None, :], NC)
        for r in range(R_BLOCK):
            full[y, 0, r, :, :, r] = cosine
            full[y, 1, r, :, :, r] = -sine
    return bf16_table(full.reshape(col_count, 2 * R_BLOCK * share, NC * R_BLOCK))


def swap_table(outer, inner, width):
    index = np.arange(outer * inner * width).reshape(outer, inner, width)
    source = np.transpose(index, (1, 0, 2)).reshape(-1)
    table = np.zeros((source.size, source.size))
    table[source, np.arange(source.size)] = 1.0
    return bf16_table(table)


def dot(a, b):
    return jnp.dot(a, b, preferred_element_type=jnp.float32)


def spectrum_kernel(pieces, x_ref, swap_ref, line_ref, cos_ref, sin_ref, re_ref, im_ref, rows):
    if pieces:
        per = LANES // NB
        for g in range(NA // per):
            parts = []
            for t in range(NC // per):
                lanes = pl.ds(t * LANES, LANES)
                parts.append(
                    jnp.concatenate([x_ref[g * per + k, :, lanes] for k in range(per)], axis=1)
                )
            moved = dot(jnp.concatenate(parts, axis=0), swap_ref[...]).astype(jnp.bfloat16)
            for t in range(NC // per):
                for j in range(per):
                    rows[pl.ds((t * per + j) * R_BLOCK, R_BLOCK), pl.ds(g * LANES, LANES)] = moved[
                        t * R_BLOCK : (t + 1) * R_BLOCK, j * LANES : (j + 1) * LANES
                    ]
    else:
        rows[...] = x_ref[...].reshape(NC * R_BLOCK, NAB)
    line = dot(line_ref[...], rows[...]).astype(jnp.bfloat16)
    half = line.shape[0] // 2
    re, im = line[:half], line[half:]
    re_ref[...] = dot(re, cos_ref[...]) + dot(im, sin_ref[...])
    im_ref[...] = dot(im, cos_ref[...]) - dot(re, sin_ref[...])


def spectrum(pieces, x, line_table):
    r_count = x.shape[1]
    cosine, sine = plane_tables()
    per = LANES // NB
    swap = swap_table(per, per, NB)
    out_rows = line_table.shape[0] // 2
    steps = r_count // R_BLOCK
    whole = lambda table: pl.BlockSpec(table.shape, lambda i: (0, 0))
    out = jax.ShapeDtypeStruct((out_rows * steps, NAB), jnp.float32)
    out_spec = pl.BlockSpec((out_rows, NAB), lambda i: (i, 0))
    return pl.pallas_call(
        functools.partial(spectrum_kernel, pieces),
        grid=(steps,),
        in_specs=[
            pl.BlockSpec((x.shape[0], R_BLOCK, x.shape[2]), lambda i: (0, i, 0)),
            whole(swap),
            whole(line_table),
            whole(cosine),
            whole(sine),
        ],
        out_specs=[out_spec, out_spec],
        out_shape=[out, out],
        scratch_shapes=[pltpu.VMEM((NC * R_BLOCK, NAB), jnp.bfloat16)],
        compiler_params=pltpu.CompilerParams(vmem_limit_bytes=48 * 1024 * 1024),
    )(x, swap, line_table, cosine, sine)


MESH = pl.DeviceIdType.MESH


def far_first(count):
    return sorted(range(1, count), key=lambda k: abs(k - count // 2))


def enter(row_count, col_count, row, col):
    barrier = pltpu.get_barrier_semaphore()
    for k in range(1, row_count):
        target = (lax.rem(row + k, row_count), col)
        pl.semaphore_signal(barrier, inc=1, device_id=target, device_id_type=MESH)
    for k in range(1, col_count):
        target = (row, lax.rem(col + k, col_count))
        pl.semaphore_signal(barrier, inc=1, device_id=target, device_id_type=MESH)
    pl.semaphore_wait(barrier, row_count + col_count - 2)


def send(src, dst, send_sem, recv_sem, target):
    return pltpu.make_async_remote_copy(
        src_ref=src,
        dst_ref=dst,
        send_sem=send_sem,
        recv_sem=recv_sem,
        device_id=target,
        device_id_type=MESH,
    )


def gather_kernel(
    row_count,
    col_count,
    inner,
    occ_ref,
    vir_ref,
    occ_slab,
    vir_slab,
    occ_out,
    vir_out,
    occ_rows,
    vir_rows,
    wave_send,
    wave_recv,
    col_send,
    col_recv,
    line_send,
    line_recv,
    group_send,
    group_recv,
    local,
):
    row, col = lax.axis_index("row"), lax.axis_index("col")
    outer = row_count // inner
    mine, seat = lax.div(row, inner), lax.rem(row, inner)
    points = occ_ref.shape[1] // row_count
    waves = ((occ_ref, occ_out), (vir_ref, vir_out))
    slabs = ((occ_slab, occ_rows), (vir_slab, vir_rows))
    enter(row_count, col_count, row, col)

    def block(index):
        return pl.ds(pl.multiple_of(index * points, LANES), points)

    own = [
        pltpu.make_async_copy(src.at[:, block(row)], dst.at[row], local.at[i])
        for i, (src, dst) in enumerate(waves)
    ]
    for copy in own:
        copy.start()

    def over_col(i, k):
        src, dst = slabs[i]
        place = dst.at[mine, seat]
        return send(src, place, col_send.at[i, k], col_recv.at[i, 0], (row, k))

    @pl.when(col == 0)
    def _():
        for i, (src, dst) in enumerate(slabs):
            for k in range(1, col_count):
                over_col(i, k).start()
            pltpu.make_async_copy(src, dst.at[mine, seat], local.at[2 + i]).start()

    def wave(i, k):
        src, dst = waves[i]
        to = lax.rem(row + k, row_count)
        return send(
            src.at[:, block(to)], dst.at[row], wave_send.at[i, k], wave_recv.at[i, k], (to, col)
        )

    order = far_first(row_count)
    half = len(order) // 2
    pending = []

    def start_waves(chosen):
        for k in chosen:
            for i in range(2):
                copy = wave(i, k)
                copy.start()
                pending.append(copy)

    start_waves(order[:1])

    @pl.when(col == 0)
    def _():
        for i, (src, dst) in enumerate(slabs):
            pltpu.make_async_copy(src, dst.at[mine, seat], local.at[2 + i]).wait()

    @pl.when(col != 0)
    def _():
        for i in range(2):
            over_col(i, 1).wait_recv()

    lines = []
    for k in range(1, outer):
        to = (lax.rem(mine + k, outer) * inner + seat, col)
        for i in range(2):
            place = slabs[i][1].at[mine, seat]
            copy = send(place, place, line_send.at[i, k], line_recv.at[i, k], to)
            copy.start()
            lines.append(copy)
    start_waves(order[1:half])
    for copy in lines:
        copy.wait_recv()
    groups = []
    for k in range(1, inner):
        to = (mine * inner + lax.rem(seat + k, inner), col)
        for i in range(2):
            place = slabs[i][1].at[:, seat]
            copy = send(place, place, group_send.at[i, k], group_recv.at[i, k], to)
            copy.start()
            groups.append(copy)
    start_waves(order[half:])
    for copy in own:
        copy.wait()
    for copy in groups:
        copy.wait()
    for copy in lines:
        copy.wait_send()

    @pl.when(col == 0)
    def _():
        for i in range(2):
            for k in range(1, col_count):
                over_col(i, k).wait_send()

    for copy in pending:
        copy.wait()


def gather(row_count, col_count, occ, vir, occ_slab, vir_slab):
    inner = 4 if row_count % 4 == 0 else 1
    points = occ.shape[1] // row_count
    window = occ_slab.shape[1]
    outer = row_count // inner
    shapes = [(row_count, w.shape[0], points) for w in (occ, vir)]
    shapes += [(outer, inner, w.shape[0], window) for w in (occ, vir)]
    dma = pltpu.SemaphoreType.DMA
    return pl.pallas_call(
        functools.partial(gather_kernel, row_count, col_count, inner),
        out_shape=[jax.ShapeDtypeStruct(shape, jnp.bfloat16) for shape in shapes],
        in_specs=[pl.BlockSpec(memory_space=pl.ANY)] * 2
        + [pl.BlockSpec(memory_space=pltpu.VMEM)] * 2,
        out_specs=[pl.BlockSpec(memory_space=pltpu.VMEM)] * 4,
        scratch_shapes=[dma((2, row_count))] * 2
        + [dma((2, col_count))] * 2
        + [dma((2, outer))] * 2
        + [dma((2, inner))] * 2
        + [dma((4,))],
        compiler_params=pltpu.CompilerParams(
            collective_id=0, has_side_effects=True, vmem_limit_bytes=32 * 1024 * 1024
        ),
    )(occ, vir, occ_slab, vir_slab)


def deliver_kernel(
    row_count, col_count, p_ref, x_ref, row_send, row_recv, col_send, col_recv, local
):
    row, col = lax.axis_index("row"), lax.axis_index("col")
    enter(row_count, col_count, row, col)
    order = far_first(row_count)
    here = x_ref.at[col, row]
    own = pltpu.make_async_copy(p_ref.at[row], here, local.at[0])
    own.start()
    rows = []
    for k in order:
        to = lax.rem(row + k, row_count)
        copy = send(p_ref.at[to], here, row_send.at[k], row_recv.at[k], (to, col))
        copy.start()
        rows.append(copy)
    forwards = []

    def forward(k, src, slot):
        for d in range(1, col_count):
            to = (row, lax.rem(col + d, col_count))
            copy = send(src, slot, col_send.at[d, k], col_recv.at[d, k], to)
            copy.start()
            forwards.append(copy)

    forward(0, p_ref.at[row], here)
    for k, copy in zip(order, rows):
        copy.wait_recv()
        slot = x_ref.at[col, lax.rem(row + row_count - k, row_count)]
        forward(k, slot, slot)
    own.wait()
    for copy in rows:
        copy.wait_send()
    for copy in forwards:
        copy.wait()


def deliver(row_count, col_count, polar):
    dma = pltpu.SemaphoreType.DMA
    return pl.pallas_call(
        functools.partial(deliver_kernel, row_count, col_count),
        out_shape=jax.ShapeDtypeStruct((col_count,) + polar.shape, jnp.bfloat16),
        in_specs=[pl.BlockSpec(memory_space=pltpu.VMEM)],
        out_specs=pl.BlockSpec(memory_space=pltpu.VMEM),
        scratch_shapes=[dma((row_count,))] * 2 + [dma((col_count, row_count))] * 2 + [dma((1,))],
        compiler_params=pltpu.CompilerParams(
            collective_id=1, has_side_effects=True, vmem_limit_bytes=32 * 1024 * 1024
        ),
    )(polar)


def on_device(rows_dev, occupied_waves, virtual_waves, occupied_decay, virtual_decay):
    row_count = lax.axis_size("row")
    col_count = lax.axis_size("col")
    nocc, nvir = occupied_decay.shape[0], virtual_decay.shape[0]
    window = rows_dev * row_count
    points = occupied_waves.shape[1] // row_count
    contract = (((0,), (0,)), ((), ()))
    factor = -1.0 / math.sqrt(nocc * nvir) / math.sqrt(NGRID)

    def slab(waves, decay):
        share = waves.shape[0]
        own = lax.dynamic_slice_in_dim(decay, lax.axis_index("row") * share, share)
        return (waves[:, :window].astype(jnp.float32) * own[:, None]).astype(jnp.bfloat16)

    plane_occ, plane_vir, occ_rows, vir_rows = gather(
        row_count,
        col_count,
        occupied_waves,
        virtual_waves,
        slab(occupied_waves, occupied_decay),
        slab(virtual_waves, virtual_decay),
    )
    plane_occ, plane_vir = plane_occ.reshape(nocc, points), plane_vir.reshape(nvir, points)
    occ_rows, vir_rows = occ_rows.reshape(nocc, window), vir_rows.reshape(nvir, window)
    green_occ = lax.dot_general(occ_rows, plane_occ, contract, preferred_element_type=jnp.float32)
    green_vir = lax.dot_general(vir_rows, plane_vir, contract, preferred_element_type=jnp.float32)
    polar = (green_occ * green_vir * factor).astype(jnp.bfloat16)
    polar = dot(polar, swap_table(points // NC, NC, 1)).astype(jnp.bfloat16)
    polar = polar.reshape(row_count, rows_dev, points)
    polar = deliver(row_count, col_count, polar)
    pieces = points == NB * NC
    if pieces:
        x = polar.reshape(col_count * row_count, rows_dev, points)
    else:
        x = polar.reshape(col_count * row_count, rows_dev, NC, points // NC)
        x = jnp.transpose(x, (2, 1, 0, 3)).reshape(NC, rows_dev, NAB)
    table = lax.dynamic_index_in_dim(line_tables(col_count), lax.axis_index("col"), 0, False)
    real_part, imag_part = spectrum(pieces, x, table)
    shape = (rows_dev, NC // col_count, NAB)
    return real_part.reshape(shape), imag_part.reshape(shape)


ROWS_DEV = 32


def solution(mesh):
    in_specs = (P("row", "col"), P("row", "col"), P(), P())
    out_specs = (P("row", "col", None), P("row", "col", None))
    return jax.shard_map(
        functools.partial(on_device, ROWS_DEV),
        mesh=mesh,
        in_specs=in_specs,
        out_specs=out_specs,
        check_vma=False,
    )
```

```python
import functools
import math

import jax
import jax.numpy as jnp
import numpy as np
from jax import lax
from jax.experimental import pallas as pl
from jax.experimental.pallas import tpu as pltpu
from jax.sharding import PartitionSpec as P

NA = 32
NB = 32
NC = 32
NAB = NA * NB
NGRID = NA * NB * NC
LANES = 128
R_BLOCK = 16


def trig(phase, length):
    angle = (phase % length) * (2.0 * math.pi / length)
    return np.cos(angle), np.sin(angle)


def bf16_table(table):
    return jnp.asarray(table.astype(np.float32)).astype(jnp.bfloat16)


def plane_tables():
    index = np.arange(NAB)
    a, b = index // NB, index % NB
    phase = a[:, None] * a[None, :] * NB + b[:, None] * b[None, :] * NA
    cosine, sine = trig(phase, NA * NB)
    return bf16_table(cosine), bf16_table(sine)


def line_tables(col_count):
    share = NC // col_count
    full = np.zeros((col_count, 2, R_BLOCK, share, NC, R_BLOCK))
    for y in range(col_count):
        kc = y * share + np.arange(share)
        cosine, sine = trig(kc[:, None] * np.arange(NC)[None, :], NC)
        for r in range(R_BLOCK):
            full[y, 0, r, :, :, r] = cosine
            full[y, 1, r, :, :, r] = -sine
    return bf16_table(full.reshape(col_count, 2 * R_BLOCK * share, NC * R_BLOCK))


def swap_table(outer, inner, width):
    index = np.arange(outer * inner * width).reshape(outer, inner, width)
    source = np.transpose(index, (1, 0, 2)).reshape(-1)
    table = np.zeros((source.size, source.size))
    table[source, np.arange(source.size)] = 1.0
    return bf16_table(table)


def dot(a, b):
    return jnp.dot(a, b, preferred_element_type=jnp.float32)


def spectrum_kernel(pieces, x_ref, swap_ref, line_ref, cos_ref, sin_ref, re_ref, im_ref, rows):
    if pieces:
        per = LANES // NB
        for g in range(NA // per):
            parts = []
            for t in range(NC // per):
                lanes = pl.ds(t * LANES, LANES)
                parts.append(
                    jnp.concatenate([x_ref[g * per + k, :, lanes] for k in range(per)], axis=1)
                )
            moved = dot(jnp.concatenate(parts, axis=0), swap_ref[...]).astype(jnp.bfloat16)
            for t in range(NC // per):
                for j in range(per):
                    rows[pl.ds((t * per + j) * R_BLOCK, R_BLOCK), pl.ds(g * LANES, LANES)] = moved[
                        t * R_BLOCK : (t + 1) * R_BLOCK, j * LANES : (j + 1) * LANES
                    ]
    else:
        rows[...] = x_ref[...].reshape(NC * R_BLOCK, NAB)
    line = dot(line_ref[...], rows[...]).astype(jnp.bfloat16)
    half = line.shape[0] // 2
    re, im = line[:half], line[half:]
    re_ref[...] = dot(re, cos_ref[...]) + dot(im, sin_ref[...])
    im_ref[...] = dot(im, cos_ref[...]) - dot(re, sin_ref[...])


def spectrum(pieces, x, line_table):
    r_count = x.shape[1]
    cosine, sine = plane_tables()
    per = LANES // NB
    swap = swap_table(per, per, NB)
    out_rows = line_table.shape[0] // 2
    steps = r_count // R_BLOCK
    whole = lambda table: pl.BlockSpec(table.shape, lambda i: (0, 0))
    out = jax.ShapeDtypeStruct((out_rows * steps, NAB), jnp.float32)
    out_spec = pl.BlockSpec((out_rows, NAB), lambda i: (i, 0))
    return pl.pallas_call(
        functools.partial(spectrum_kernel, pieces),
        grid=(steps,),
        in_specs=[
            pl.BlockSpec((x.shape[0], R_BLOCK, x.shape[2]), lambda i: (0, i, 0)),
            whole(swap),
            whole(line_table),
            whole(cosine),
            whole(sine),
        ],
        out_specs=[out_spec, out_spec],
        out_shape=[out, out],
        scratch_shapes=[pltpu.VMEM((NC * R_BLOCK, NAB), jnp.bfloat16)],
        compiler_params=pltpu.CompilerParams(vmem_limit_bytes=48 * 1024 * 1024),
    )(x, swap, line_table, cosine, sine)


MESH = pl.DeviceIdType.MESH


def flip(index, mask):
    bits = [1 << bit for bit in range(mask.bit_length()) if mask >> bit & 1]
    for bit in bits:
        index = index + bit - 2 * bit * lax.rem(lax.div(index, bit), 2)
    return index


def group_size(row_count):
    return 4 if row_count % 4 == 0 else 1


def enter(row_count, col_count, row, col):
    barrier = pltpu.get_barrier_semaphore()
    for k in range(1, row_count):
        target = (lax.rem(row + k, row_count), col)
        pl.semaphore_signal(barrier, inc=1, device_id=target, device_id_type=MESH)
    for k in range(1, col_count):
        target = (row, lax.rem(col + k, col_count))
        pl.semaphore_signal(barrier, inc=1, device_id=target, device_id_type=MESH)
    pl.semaphore_wait(barrier, row_count + col_count - 2)


def send(src, dst, send_sem, recv_sem, target):
    return pltpu.make_async_remote_copy(
        src_ref=src,
        dst_ref=dst,
        send_sem=send_sem,
        recv_sem=recv_sem,
        device_id=target,
        device_id_type=MESH,
    )


def gather_kernel(
    row_count,
    col_count,
    inner,
    occ_ref,
    vir_ref,
    occ_slab,
    vir_slab,
    occ_out,
    vir_out,
    occ_rows,
    vir_rows,
    wave_send,
    wave_recv,
    col_send,
    col_recv,
    line_send,
    line_recv,
    group_send,
    group_recv,
    local,
):
    row, col = lax.axis_index("row"), lax.axis_index("col")
    outer = row_count // inner
    mine, seat = lax.div(row, inner), lax.rem(row, inner)
    points = occ_ref.shape[1] // row_count
    waves = ((occ_ref, occ_out), (vir_ref, vir_out))
    slabs = ((occ_slab, occ_rows), (vir_slab, vir_rows))
    enter(row_count, col_count, row, col)

    def block(index):
        return pl.ds(pl.multiple_of(index * points, LANES), points)

    own = [
        pltpu.make_async_copy(src.at[:, block(row)], dst.at[row], local.at[i])
        for i, (src, dst) in enumerate(waves)
    ]
    for copy in own:
        copy.start()

    def over_col(i, k):
        src, dst = slabs[i]
        place = dst.at[mine, seat]
        return send(src, place, col_send.at[i, k], col_recv.at[i, 0], (row, k))

    @pl.when(col == 0)
    def _():
        for i, (src, dst) in enumerate(slabs):
            for k in range(1, col_count):
                over_col(i, k).start()
            pltpu.make_async_copy(src, dst.at[mine, seat], local.at[2 + i]).start()

    pending = []

    def start_waves(far, steps=range(inner)):
        for step in steps:
            if far == 0 and step == 0:
                continue
            k = far * inner + step
            there = flip(mine, far)
            to = there * inner + lax.rem(seat + step, inner)
            for i, (src, dst) in enumerate(waves):
                copy = send(
                    src.at[:, block(to)],
                    dst.at[row],
                    wave_send.at[i, k],
                    wave_recv.at[i, k],
                    (to, col),
                )
                copy.start()
                pending.append(copy)

    start_waves(0)

    @pl.when(col == 0)
    def _():
        for i, (src, dst) in enumerate(slabs):
            pltpu.make_async_copy(src, dst.at[mine, seat], local.at[2 + i]).wait()

    @pl.when(col != 0)
    def _():
        for i in range(2):
            over_col(i, 1).wait_recv()

    lines = []
    bits = [1 << bit for bit in reversed(range((outer - 1).bit_length()))]
    early = inner // 2

    def double(held, bit):
        to = (flip(mine, bit) * inner + seat, col)
        started = []
        for mask in held:
            for i in range(2):
                place = slabs[i][1].at[flip(mine, mask), seat]
                k = bit + mask
                started.append(send(place, place, line_send.at[i, k], line_recv.at[i, k], to))
        for copy in started:
            copy.start()
        lines.extend(started)
        return started

    held = [0]
    for number, bit in enumerate(bits):
        started = double(held, bit)
        if number == 0:
            start_waves(bits[0], range(early))
        held = held + [mask + bit for mask in held]
        if number == len(bits) - 1:
            for far in range(1, bits[0]):
                start_waves(far)
            start_waves(bits[0], range(early, inner))
        for copy in started:
            copy.wait_recv()
    groups = []
    for k in range(1, inner):
        to = (mine * inner + lax.rem(seat + k, inner), col)
        for i in range(2):
            place = slabs[i][1].at[:, seat]
            copy = send(place, place, group_send.at[i, k], group_recv.at[i, k], to)
            copy.start()
            groups.append(copy)
    for far in range(bits[0] + 1 if bits else 1, outer):
        start_waves(far)
    for copy in own:
        copy.wait()
    for copy in groups:
        copy.wait()
    for copy in lines:
        copy.wait_send()

    @pl.when(col == 0)
    def _():
        for i in range(2):
            for k in range(1, col_count):
                over_col(i, k).wait_send()

    for copy in pending:
        copy.wait()


def gather(row_count, col_count, occ, vir, occ_slab, vir_slab):
    inner = group_size(row_count)
    points = occ.shape[1] // row_count
    window = occ_slab.shape[1]
    outer = row_count // inner
    shapes = [(row_count, w.shape[0], points) for w in (occ, vir)]
    shapes += [(outer, inner, w.shape[0], window) for w in (occ, vir)]
    dma = pltpu.SemaphoreType.DMA
    return pl.pallas_call(
        functools.partial(gather_kernel, row_count, col_count, inner),
        out_shape=[jax.ShapeDtypeStruct(shape, jnp.bfloat16) for shape in shapes],
        in_specs=[pl.BlockSpec(memory_space=pl.ANY)] * 2
        + [pl.BlockSpec(memory_space=pltpu.VMEM)] * 2,
        out_specs=[pl.BlockSpec(memory_space=pltpu.VMEM)] * 4,
        scratch_shapes=[dma((2, row_count))] * 2
        + [dma((2, col_count))] * 2
        + [dma((2, outer))] * 2
        + [dma((2, inner))] * 2
        + [dma((4,))],
        compiler_params=pltpu.CompilerParams(
            collective_id=0, has_side_effects=True, vmem_limit_bytes=32 * 1024 * 1024
        ),
    )(occ, vir, occ_slab, vir_slab)


def deliver_kernel(
    row_count, col_count, p_ref, x_ref, row_send, row_recv, col_send, col_recv, local
):
    row, col = lax.axis_index("row"), lax.axis_index("col")
    enter(row_count, col_count, row, col)
    inner = group_size(row_count)
    mine, seat = lax.div(row, inner), lax.rem(row, inner)
    here = x_ref.at[col, row]
    own = pltpu.make_async_copy(p_ref.at[row], here, local.at[0])
    own.start()
    rows = []
    order = range(1, row_count)
    for k in order:
        to = flip(mine, k // inner) * inner + lax.rem(seat + k % inner, inner)
        copy = send(p_ref.at[to], here, row_send.at[k], row_recv.at[k], (to, col))
        copy.start()
        rows.append(copy)
    forwards = []

    def forward(k, src, slot):
        for d in range(1, col_count):
            to = (row, lax.rem(col + d, col_count))
            copy = send(src, slot, col_send.at[d, k], col_recv.at[d, k], to)
            copy.start()
            forwards.append(copy)

    forward(0, p_ref.at[row], here)
    for k, copy in zip(order, rows):
        copy.wait_recv()
        source = flip(mine, k // inner) * inner + lax.rem(seat + inner - k % inner, inner)
        slot = x_ref.at[col, source]
        forward(k, slot, slot)
    own.wait()
    for copy in rows:
        copy.wait_send()
    for copy in forwards:
        copy.wait()


def deliver(row_count, col_count, polar):
    dma = pltpu.SemaphoreType.DMA
    return pl.pallas_call(
        functools.partial(deliver_kernel, row_count, col_count),
        out_shape=jax.ShapeDtypeStruct((col_count,) + polar.shape, jnp.bfloat16),
        in_specs=[pl.BlockSpec(memory_space=pltpu.VMEM)],
        out_specs=pl.BlockSpec(memory_space=pltpu.VMEM),
        scratch_shapes=[dma((row_count,))] * 2 + [dma((col_count, row_count))] * 2 + [dma((1,))],
        compiler_params=pltpu.CompilerParams(
            collective_id=1, has_side_effects=True, vmem_limit_bytes=32 * 1024 * 1024
        ),
    )(polar)


def on_device(rows_dev, occupied_waves, virtual_waves, occupied_decay, virtual_decay):
    row_count = lax.axis_size("row")
    col_count = lax.axis_size("col")
    nocc, nvir = occupied_decay.shape[0], virtual_decay.shape[0]
    window = rows_dev * row_count
    points = occupied_waves.shape[1] // row_count
    contract = (((0,), (0,)), ((), ()))
    factor = -1.0 / math.sqrt(nocc * nvir) / math.sqrt(NGRID)

    def slab(waves, decay):
        share = waves.shape[0]
        own = lax.dynamic_slice_in_dim(decay, lax.axis_index("row") * share, share)
        return (waves[:, :window].astype(jnp.float32) * own[:, None]).astype(jnp.bfloat16)

    plane_occ, plane_vir, occ_rows, vir_rows = gather(
        row_count,
        col_count,
        occupied_waves,
        virtual_waves,
        slab(occupied_waves, occupied_decay),
        slab(virtual_waves, virtual_decay),
    )
    plane_occ, plane_vir = plane_occ.reshape(nocc, points), plane_vir.reshape(nvir, points)
    occ_rows, vir_rows = occ_rows.reshape(nocc, window), vir_rows.reshape(nvir, window)
    green_occ = lax.dot_general(occ_rows, plane_occ, contract, preferred_element_type=jnp.float32)
    green_vir = lax.dot_general(vir_rows, plane_vir, contract, preferred_element_type=jnp.float32)
    polar = (green_occ * green_vir * factor).astype(jnp.bfloat16)
    polar = dot(polar, swap_table(points // NC, NC, 1)).astype(jnp.bfloat16)
    polar = polar.reshape(row_count, rows_dev, points)
    polar = deliver(row_count, col_count, polar)
    pieces = points == NB * NC
    if pieces:
        x = polar.reshape(col_count * row_count, rows_dev, points)
    else:
        x = polar.reshape(col_count * row_count, rows_dev, NC, points // NC)
        x = jnp.transpose(x, (2, 1, 0, 3)).reshape(NC, rows_dev, NAB)
    table = lax.dynamic_index_in_dim(line_tables(col_count), lax.axis_index("col"), 0, False)
    real_part, imag_part = spectrum(pieces, x, table)
    shape = (rows_dev, NC // col_count, NAB)
    return real_part.reshape(shape), imag_part.reshape(shape)


ROWS_DEV = 32


def solution(mesh):
    in_specs = (P("row", "col"), P("row", "col"), P(), P())
    out_specs = (P("row", "col", None), P("row", "col", None))
    return jax.shard_map(
        functools.partial(on_device, ROWS_DEV),
        mesh=mesh,
        in_specs=in_specs,
        out_specs=out_specs,
        check_vma=False,
    )
```

```python
import functools
import math

import jax
import jax.numpy as jnp
import numpy as np
from jax import lax
from jax.experimental import pallas as pl
from jax.experimental.pallas import tpu as pltpu
from jax.sharding import PartitionSpec as P

NA = 32
NB = 32
NC = 32
NAB = NA * NB
NGRID = NA * NB * NC
LANES = 128
R_BLOCK = 16


def trig(phase, length):
    angle = (phase % length) * (2.0 * math.pi / length)
    return np.cos(angle), np.sin(angle)


def bf16_table(table):
    return jnp.asarray(table.astype(np.float32)).astype(jnp.bfloat16)


def plane_tables():
    index = np.arange(NAB)
    a, b = index // NB, index % NB
    phase = a[:, None] * a[None, :] * NB + b[:, None] * b[None, :] * NA
    cosine, sine = trig(phase, NA * NB)
    return bf16_table(cosine), bf16_table(sine)


def line_tables(col_count):
    share = NC // col_count
    full = np.zeros((col_count, 2, R_BLOCK, share, NC, R_BLOCK))
    for y in range(col_count):
        kc = y * share + np.arange(share)
        cosine, sine = trig(kc[:, None] * np.arange(NC)[None, :], NC)
        for r in range(R_BLOCK):
            full[y, 0, r, :, :, r] = cosine
            full[y, 1, r, :, :, r] = -sine
    return bf16_table(full.reshape(col_count, 2 * R_BLOCK * share, NC * R_BLOCK))


def swap_table(outer, inner, width):
    index = np.arange(outer * inner * width).reshape(outer, inner, width)
    source = np.transpose(index, (1, 0, 2)).reshape(-1)
    table = np.zeros((source.size, source.size))
    table[source, np.arange(source.size)] = 1.0
    return bf16_table(table)


def dot(a, b):
    return jnp.dot(a, b, preferred_element_type=jnp.float32)


def spectrum_kernel(pieces, x_ref, swap_ref, line_ref, cos_ref, sin_ref, re_ref, im_ref, rows):
    if pieces:
        per = LANES // NB
        for g in range(NA // per):
            parts = []
            for t in range(NC // per):
                lanes = pl.ds(t * LANES, LANES)
                parts.append(
                    jnp.concatenate([x_ref[g * per + k, :, lanes] for k in range(per)], axis=1)
                )
            moved = dot(jnp.concatenate(parts, axis=0), swap_ref[...]).astype(jnp.bfloat16)
            for t in range(NC // per):
                for j in range(per):
                    rows[pl.ds((t * per + j) * R_BLOCK, R_BLOCK), pl.ds(g * LANES, LANES)] = moved[
                        t * R_BLOCK : (t + 1) * R_BLOCK, j * LANES : (j + 1) * LANES
                    ]
    else:
        rows[...] = x_ref[...].reshape(NC * R_BLOCK, NAB)
    line = dot(line_ref[lax.axis_index("col")], rows[...]).astype(jnp.bfloat16)
    half = line.shape[0] // 2
    re, im = line[:half], line[half:]
    re_ref[...] = dot(re, cos_ref[...]) + dot(im, sin_ref[...])
    im_ref[...] = dot(im, cos_ref[...]) - dot(re, sin_ref[...])


def spectrum(pieces, x, line_table):
    r_count = x.shape[1]
    cosine, sine = plane_tables()
    per = LANES // NB
    swap = swap_table(per, per, NB)
    out_rows = line_table.shape[1] // 2
    steps = r_count // R_BLOCK
    whole = lambda table: pl.BlockSpec(table.shape, lambda i: (0,) * table.ndim)
    out = jax.ShapeDtypeStruct((out_rows * steps, NAB), jnp.float32)
    out_spec = pl.BlockSpec((out_rows, NAB), lambda i: (i, 0))
    return pl.pallas_call(
        functools.partial(spectrum_kernel, pieces),
        grid=(steps,),
        in_specs=[
            pl.BlockSpec((x.shape[0], R_BLOCK, x.shape[2]), lambda i: (0, i, 0)),
            whole(swap),
            whole(line_table),
            whole(cosine),
            whole(sine),
        ],
        out_specs=[out_spec, out_spec],
        out_shape=[out, out],
        scratch_shapes=[pltpu.VMEM((NC * R_BLOCK, NAB), jnp.bfloat16)],
        compiler_params=pltpu.CompilerParams(vmem_limit_bytes=48 * 1024 * 1024),
    )(x, swap, line_table, cosine, sine)


MESH = pl.DeviceIdType.MESH


def flip(index, mask):
    bits = [1 << bit for bit in range(mask.bit_length()) if mask >> bit & 1]
    for bit in bits:
        index = index + bit - 2 * bit * lax.rem(lax.div(index, bit), 2)
    return index


def group_size(row_count):
    return 4 if row_count % 4 == 0 else 1


def enter(row_count, col_count, row, col):
    barrier = pltpu.get_barrier_semaphore()
    for k in range(1, row_count):
        target = (lax.rem(row + k, row_count), col)
        pl.semaphore_signal(barrier, inc=1, device_id=target, device_id_type=MESH)
    for k in range(1, col_count):
        target = (row, lax.rem(col + k, col_count))
        pl.semaphore_signal(barrier, inc=1, device_id=target, device_id_type=MESH)
    pl.semaphore_wait(barrier, row_count + col_count - 2)


def send(src, dst, send_sem, recv_sem, target):
    return pltpu.make_async_remote_copy(
        src_ref=src,
        dst_ref=dst,
        send_sem=send_sem,
        recv_sem=recv_sem,
        device_id=target,
        device_id_type=MESH,
    )


def gather_kernel(
    row_count,
    col_count,
    inner,
    occ_ref,
    vir_ref,
    occ_slab,
    vir_slab,
    occ_out,
    vir_out,
    occ_rows,
    vir_rows,
    wave_send,
    wave_recv,
    col_send,
    col_recv,
    line_send,
    line_recv,
    group_send,
    group_recv,
    local,
):
    row, col = lax.axis_index("row"), lax.axis_index("col")
    outer = row_count // inner
    mine, seat = lax.div(row, inner), lax.rem(row, inner)
    points = occ_ref.shape[1] // row_count
    waves = ((occ_ref, occ_out), (vir_ref, vir_out))
    slabs = ((occ_slab, occ_rows), (vir_slab, vir_rows))
    enter(row_count, col_count, row, col)

    def block(index):
        return pl.ds(pl.multiple_of(index * points, LANES), points)

    own = [
        pltpu.make_async_copy(src.at[:, block(row)], dst.at[row], local.at[i])
        for i, (src, dst) in enumerate(waves)
    ]
    for copy in own:
        copy.start()

    def over_col(i, k):
        src, dst = slabs[i]
        place = dst.at[mine, seat]
        return send(src, place, col_send.at[i, k], col_recv.at[i, 0], (row, k))

    @pl.when(col == 0)
    def _():
        for i, (src, dst) in enumerate(slabs):
            for k in range(1, col_count):
                over_col(i, k).start()
            pltpu.make_async_copy(src, dst.at[mine, seat], local.at[2 + i]).start()

    pending = []

    def start_waves(far, steps=range(inner)):
        for step in steps:
            if far == 0 and step == 0:
                continue
            k = far * inner + step
            there = flip(mine, far)
            to = there * inner + lax.rem(seat + step, inner)
            for i, (src, dst) in enumerate(waves):
                copy = send(
                    src.at[:, block(to)],
                    dst.at[row],
                    wave_send.at[i, k],
                    wave_recv.at[i, k],
                    (to, col),
                )
                copy.start()
                pending.append(copy)

    start_waves(0)

    @pl.when(col == 0)
    def _():
        for i, (src, dst) in enumerate(slabs):
            pltpu.make_async_copy(src, dst.at[mine, seat], local.at[2 + i]).wait()

    @pl.when(col != 0)
    def _():
        for i in range(2):
            over_col(i, 1).wait_recv()

    lines = []
    bits = [1 << bit for bit in reversed(range((outer - 1).bit_length()))]
    early = inner // 2

    def double(held, bit):
        to = (flip(mine, bit) * inner + seat, col)
        started = []
        for mask in held:
            for i in range(2):
                place = slabs[i][1].at[flip(mine, mask), seat]
                k = bit + mask
                started.append(send(place, place, line_send.at[i, k], line_recv.at[i, k], to))
        for copy in started:
            copy.start()
        lines.extend(started)
        return started

    held = [0]
    for number, bit in enumerate(bits):
        started = double(held, bit)
        if number == 0:
            start_waves(bits[0], range(early))
        held = held + [mask + bit for mask in held]
        if number == len(bits) - 1:
            for far in range(1, bits[0]):
                start_waves(far)
            start_waves(bits[0], range(early, inner))
        for copy in started:
            copy.wait_recv()
    groups = []
    for k in range(1, inner):
        to = (mine * inner + lax.rem(seat + k, inner), col)
        for i in range(2):
            place = slabs[i][1].at[:, seat]
            copy = send(place, place, group_send.at[i, k], group_recv.at[i, k], to)
            copy.start()
            groups.append(copy)
    for far in range(bits[0] + 1 if bits else 1, outer):
        start_waves(far)
    for copy in own:
        copy.wait()
    for copy in groups:
        copy.wait()
    for copy in lines:
        copy.wait_send()

    @pl.when(col == 0)
    def _():
        for i in range(2):
            for k in range(1, col_count):
                over_col(i, k).wait_send()

    for copy in pending:
        copy.wait()


def gather(row_count, col_count, occ, vir, occ_slab, vir_slab):
    inner = group_size(row_count)
    points = occ.shape[1] // row_count
    window = occ_slab.shape[1]
    outer = row_count // inner
    shapes = [(row_count, w.shape[0], points) for w in (occ, vir)]
    shapes += [(outer, inner, w.shape[0], window) for w in (occ, vir)]
    dma = pltpu.SemaphoreType.DMA
    return pl.pallas_call(
        functools.partial(gather_kernel, row_count, col_count, inner),
        out_shape=[jax.ShapeDtypeStruct(shape, jnp.bfloat16) for shape in shapes],
        in_specs=[pl.BlockSpec(memory_space=pltpu.HBM)] * 2
        + [pl.BlockSpec(memory_space=pltpu.VMEM)] * 2,
        out_specs=[pl.BlockSpec(memory_space=pltpu.VMEM)] * 4,
        scratch_shapes=[dma((2, row_count))] * 2
        + [dma((2, col_count))] * 2
        + [dma((2, outer))] * 2
        + [dma((2, inner))] * 2
        + [dma((4,))],
        compiler_params=pltpu.CompilerParams(
            collective_id=0, has_side_effects=True, vmem_limit_bytes=32 * 1024 * 1024
        ),
    )(occ, vir, occ_slab, vir_slab)


def deliver_kernel(
    row_count, col_count, p_ref, x_ref, row_send, row_recv, col_send, col_recv, local
):
    row, col = lax.axis_index("row"), lax.axis_index("col")
    enter(row_count, col_count, row, col)
    inner = group_size(row_count)
    mine, seat = lax.div(row, inner), lax.rem(row, inner)
    here = x_ref.at[col, row]
    own = pltpu.make_async_copy(p_ref.at[row], here, local.at[0])
    own.start()
    rows = []
    order = range(1, row_count)
    for k in order:
        to = flip(mine, k // inner) * inner + lax.rem(seat + k % inner, inner)
        copy = send(p_ref.at[to], here, row_send.at[k], row_recv.at[k], (to, col))
        copy.start()
        rows.append(copy)
    forwards = []

    def forward(k, src, slot):
        for d in range(1, col_count):
            to = (row, lax.rem(col + d, col_count))
            copy = send(src, slot, col_send.at[d, k], col_recv.at[d, k], to)
            copy.start()
            forwards.append(copy)

    forward(0, p_ref.at[row], here)
    for k, copy in zip(order, rows):
        copy.wait_recv()
        source = flip(mine, k // inner) * inner + lax.rem(seat + inner - k % inner, inner)
        slot = x_ref.at[col, source]
        forward(k, slot, slot)
    own.wait()
    for copy in rows:
        copy.wait_send()
    for copy in forwards:
        copy.wait()


def deliver(row_count, col_count, polar):
    dma = pltpu.SemaphoreType.DMA
    return pl.pallas_call(
        functools.partial(deliver_kernel, row_count, col_count),
        out_shape=jax.ShapeDtypeStruct((col_count,) + polar.shape, jnp.bfloat16),
        in_specs=[pl.BlockSpec(memory_space=pltpu.VMEM)],
        out_specs=pl.BlockSpec(memory_space=pltpu.VMEM),
        scratch_shapes=[dma((row_count,))] * 2 + [dma((col_count, row_count))] * 2 + [dma((1,))],
        cost_estimate=pl.CostEstimate(
            flops=0, bytes_accessed=32 * polar.size * col_count, transcendentals=0
        ),
        compiler_params=pltpu.CompilerParams(
            collective_id=1, has_side_effects=True, vmem_limit_bytes=32 * 1024 * 1024
        ),
    )(polar)


def on_device(rows_dev, occupied_waves, virtual_waves, occupied_decay, virtual_decay):
    row_count = lax.axis_size("row")
    col_count = lax.axis_size("col")
    nocc, nvir = occupied_decay.shape[0], virtual_decay.shape[0]
    window = rows_dev * row_count
    points = occupied_waves.shape[1] // row_count
    contract = (((0,), (0,)), ((), ()))
    factor = -1.0 / math.sqrt(nocc * nvir) / math.sqrt(NGRID)

    def slab(waves, decay):
        share = waves.shape[0]
        own = lax.dynamic_slice_in_dim(decay, lax.axis_index("row") * share, share)
        return (waves[:, :window].astype(jnp.float32) * own[:, None]).astype(jnp.bfloat16)

    plane_occ, plane_vir, occ_rows, vir_rows = gather(
        row_count,
        col_count,
        occupied_waves,
        virtual_waves,
        slab(occupied_waves, occupied_decay),
        slab(virtual_waves, virtual_decay),
    )
    plane_occ, plane_vir = plane_occ.reshape(nocc, points), plane_vir.reshape(nvir, points)
    occ_rows, vir_rows = occ_rows.reshape(nocc, window), vir_rows.reshape(nvir, window)
    green_occ = lax.dot_general(occ_rows, plane_occ, contract, preferred_element_type=jnp.float32)
    green_vir = lax.dot_general(vir_rows, plane_vir, contract, preferred_element_type=jnp.float32)
    polar = (green_occ * green_vir * factor).astype(jnp.bfloat16)
    polar = dot(polar, swap_table(points // NC, NC, 1)).astype(jnp.bfloat16)
    polar = polar.reshape(row_count, rows_dev, points)
    polar = deliver(row_count, col_count, polar)
    pieces = points == NB * NC
    if pieces:
        x = polar.reshape(col_count * row_count, rows_dev, points)
    else:
        x = polar.reshape(col_count * row_count, rows_dev, NC, points // NC)
        x = jnp.transpose(x, (2, 1, 0, 3)).reshape(NC, rows_dev, NAB)
    real_part, imag_part = spectrum(pieces, x, line_tables(col_count))
    shape = (rows_dev, NC // col_count, NAB)
    return real_part.reshape(shape), imag_part.reshape(shape)


ROWS_DEV = 32


def solution(mesh):
    in_specs = (P("row", "col"), P("row", "col"), P(), P())
    out_specs = (P("row", "col", None), P("row", "col", None))
    return jax.shard_map(
        functools.partial(on_device, ROWS_DEV),
        mesh=mesh,
        in_specs=in_specs,
        out_specs=out_specs,
        check_vma=False,
    )
```
